32 devices in a mesh: dp: 4 (over y, x), expert: 4 (over z), tensor: 2 (over core).
Axes of the slice: x: 2, y: 2, z: 4, core: 2. Of those that a mesh axis runs over, the one named last changes fastest.
Arguments:
- tokens: bfloat16 [1, 256, 3584], P(None, ('dp', 'expert'), 'tensor'), may hold values from -6 to 6
- gate_weight: bfloat16 [16, 3584, 1024], P(('dp', 'expert'), None, 'tensor'), may hold values from -0.09375 to 0.09375
- up_weight: bfloat16 [16, 3584, 1024], P(('dp', 'expert'), None, 'tensor'), may hold values from -0.09375 to 0.09375
- down_weight: bfloat16 [16, 1024, 3584], P(('dp', 'expert'), 'tensor'), may hold values from -0.1875 to 0.1875
- expert_ids: int32 [1, 256, 8], P(None, ('dp', 'expert')), may hold values from 0 to 15, all different within a row; in each aligned block of 16 rows (0 to 15, 16 to 31, ..., all dimensions but the last counted through in order) at most 16 rows name the same one
- gate_codes: int32 [1, 256, 8], P(None, ('dp', 'expert')), may hold values from 1 to 32767
Outputs:
- mixed: bfloat16 [1, 256, 3584], P(None, ('dp', 'expert'), 'tensor')
The draws below stay inside these ranges and needn't reach their ends.
Inputs may be any that keep to these rules, and one draw needn't show every extreme that they name: `expert_ids`: the 8 experts of one token differ. For every step, of the 16 tokens that one index of dp+expert holds, no expert is named by more than 16.
All inputs are finite; a program needn't handle non-finite values.
Results may differ from the reference program's by a relative error of at most 0.0095.
Values may be sent and summed in bfloat16 or wider, within the bound.
A program may use at most 64 MiB of HBM per device.

```python
import math
import jax
import jax.numpy as jnp
import numpy as np
from jax import lax

D = 3584
FF = 1024
TOP = 8
STEPS = 1
TOK = 16
EXPERTS = 16
MOST = 16
TOKENS = 256
N_DP = 4
N_EXPERT = 4
N_TENSOR = 2


def with_ends(array, own_key, smallest, high):
    place = [jax.random.randint(jax.random.fold_in(own_key, axis), (), 0, length) for axis, length in enumerate(array.shape)]
    main_axis = array.shape.index(max(array.shape))
    beside = place[:main_axis] + [(place[main_axis] + 1) % array.shape[main_axis]] + place[main_axis + 1:]
    return array.at[tuple(place)].set(smallest).at[tuple(beside)].set(high)


def steps_of(key, shape, shards, low, top_value):
    loudness, own = 1.0, jax.random.fold_in(key, 6)
    for position, parts in shards:
        draws = jnp.exp(jax.random.uniform(jax.random.fold_in(own, position), (parts,), jnp.float32, low / len(shards), top_value / len(shards)))
        loudness = loudness * jnp.repeat(draws, shape[position] // parts).reshape([-1 if axis == position else 1 for axis in range(len(shape))])
    return loudness


def shared_out(stream_key, own, number, rows, number_of, top, bound, skew):
    ranking = jax.random.permutation(stream_key, number_of)
    crowded, common = load_shares(number_of, rows * top, bound, skew, True), load_shares(number_of, rows * top, bound, skew, False)
    places = jnp.arange(number_of)

    def named(tallies, rotation):
        used = int((tallies > 0).sum())
        fixed = max(1, used // 4)
        moved = fixed + (places - fixed + rotation * (used - fixed)) % max(1, number_of - fixed)
        return jnp.zeros((number_of,), jnp.int32).at[ranking[jnp.where(places < fixed, places, moved)]].set(jnp.asarray(tallies, jnp.int32))

    tallies = jnp.where(number % 4 == 0, named(crowded, number // 4), named(common, number - number // 4 - 1))
    mixed = jax.random.permutation(jax.random.fold_in(own, 3), number_of)
    source_of, taker = mixed[0:number_of // 2 * 2:2], mixed[1:number_of // 2 * 2:2]
    margin = jnp.minimum(tallies[source_of] - 1, bound - tallies[taker]) // 2
    margin = jnp.where((source_of == ranking[0]) | (taker == ranking[0]) | (tallies[taker] == 0), 0, jnp.maximum(margin, 0))
    moved = jax.random.randint(jax.random.fold_in(own, 4), (number_of // 2,), 0, 1 << 20) % (margin + 1)
    tallies = tallies.at[source_of].add(-moved).at[taker].add(moved)
    members = jnp.searchsorted(jnp.cumsum(tallies), jnp.arange(rows * top), side="right").astype(jnp.int32)
    grid = members.reshape(top, rows).T
    grid = grid[jax.random.permutation(jax.random.fold_in(own, 1), rows)]
    rotation = jax.random.randint(jax.random.fold_in(own, 2), (rows, 1), 0, top)
    return jnp.take_along_axis(grid, (jnp.arange(top)[None, :] + rotation) % top, axis=1)


def load_shares(amount, total, bound, slope, full):
    weights = [(1 << 20) // math.isqrt(grade ** slope) + 1 for grade in range(1, amount + 1)]
    largest = bound if full else min(bound, max(-(-total // amount), total * weights[0] // sum(weights)))
    least = 1 if total - largest >= amount - 1 else 0
    given, spare = [largest] + [least] * (amount - 1), total - largest - least * (amount - 1)
    while spare > 0:
        free = [i for i in range(1, amount) if given[i] < largest] or [i for i in range(1, amount) if given[i] < bound]
        pool, left = sum([weights[i] for i in free]), spare
        for i in free:
            extra = min(bound - given[i], max(1, left * weights[i] // pool), spare)
            given[i] = given[i] + extra
            spare = spare - extra
    return np.array(given)


def noise(own_key, extent, spread, bound, shards=(), kind=jnp.bfloat16):
    level = steps_of(own_key, extent, shards, -0.22, 0.18) if shards else 1.0
    values = jax.random.normal(own_key, extent, jnp.float32) * spread * level
    return jnp.minimum(jnp.maximum(values, -bound), bound).astype(kind)


def setup_inputs(seed: int = 0) -> dict:
    keys = jax.random.split(jax.random.key(seed), 7)
    tokens = noise(keys[0], (STEPS, TOKENS, D), 1.0, 6.0, ((1, 16), (2, 2)))
    gate_weight = noise(keys[1], (EXPERTS, D, FF), D ** -0.5, 0.09375, ((0, 16), (2, 2)))
    up_weight = noise(keys[2], (EXPERTS, D, FF), D ** -0.5, 0.09375, ((0, 16), (2, 2)))
    down_weight = noise(keys[3], (EXPERTS, FF, D), FF ** -0.5, 0.1875, ((0, 16), (1, 2)))
    expert_ids_keys = jax.random.split(jax.random.fold_in(keys[4], 1), STEPS * TOKENS // TOK)
    expert_ids_turns = jax.random.permutation(jax.random.fold_in(keys[4], 3), STEPS * TOKENS // TOK)
    expert_ids = jax.vmap(lambda own, number: shared_out(jax.random.fold_in(keys[4], 2), own, number, TOK, EXPERTS, TOP, MOST, 2))(expert_ids_keys, expert_ids_turns).reshape((STEPS, TOKENS, TOP))
    gate_codes = with_ends(jax.random.randint(keys[5], (STEPS, TOKENS, TOP), 1, 32768), jax.random.fold_in(keys[5], 1), 1, 32767).astype(jnp.int32)
    return {"tokens": tokens, "gate_weight": gate_weight, "up_weight": up_weight, "down_weight": down_weight, "expert_ids": expert_ids, "gate_codes": gate_codes}


def reference(tokens, gate_weight, up_weight, down_weight, expert_ids, gate_codes):
    pair_count = STEPS * TOKENS * TOP
    flat_tokens = tokens.reshape(STEPS * TOKENS, D)
    flat_ids = expert_ids.reshape(pair_count).astype(jnp.int32)
    codes = gate_codes.astype(jnp.float32)
    shares = (codes / jnp.sum(codes, axis=2, keepdims=True)).reshape(pair_count)
    capacity = STEPS * N_DP * N_EXPERT * MOST
    half_units = FF // N_TENSOR

    def one_expert(expert, total):
        chosen = jnp.nonzero(flat_ids == expert, size=capacity, fill_value=pair_count)[0].astype(jnp.int32)
        valid = chosen < pair_count
        clipped = jnp.minimum(chosen, pair_count - 1).astype(jnp.int32)
        token_rows = (clipped // TOP).astype(jnp.int32)
        inputs = flat_tokens[token_rows]
        w_gate = lax.dynamic_index_in_dim(gate_weight, expert, 0, keepdims=False)
        w_up = lax.dynamic_index_in_dim(up_weight, expert, 0, keepdims=False)
        w_down = lax.dynamic_index_in_dim(down_weight, expert, 0, keepdims=False)
        gated = jnp.dot(inputs, w_gate, preferred_element_type=jnp.float32)
        lifted = jnp.dot(inputs, w_up, preferred_element_type=jnp.float32)
        hidden = (jax.nn.silu(gated) * lifted).astype(jnp.bfloat16)
        summed = jnp.zeros((capacity, D), jnp.float32)
        for group in range(N_TENSOR):
            piece = jnp.dot(hidden[:, group * half_units:(group + 1) * half_units],
                            w_down[group * half_units:(group + 1) * half_units],
                            preferred_element_type=jnp.float32)
            summed = summed + lax.optimization_barrier(piece.astype(jnp.bfloat16)).astype(jnp.float32)
        expert_out = lax.optimization_barrier(summed.astype(jnp.bfloat16)).astype(jnp.float32)
        scale = jnp.where(valid, shares[clipped], jnp.zeros((capacity,), jnp.float32))
        return total.at[token_rows].add(scale[:, None] * expert_out)

    total = lax.fori_loop(0, N_DP * N_EXPERT, one_expert, jnp.zeros((STEPS * TOKENS, D), jnp.float32))
    return total.astype(jnp.bfloat16).reshape(STEPS, TOKENS, D)
```

```python
import functools
import jax
import jax.numpy as jnp
from jax import lax
from jax.experimental import pallas as pl
from jax.experimental.pallas import tpu as pltpu
from jax.sharding import PartitionSpec as P

MESH = pl.DeviceIdType.MESH
LANES = 128
ORDER = (
    "F10", "F11", "F20", "F12", "F21", "F30", "F13", "F22", "F31", "C0", "F23", "F32", "C1", "R10",
    "F33", "C2", "R11", "R20", "C3", "R12", "R21", "R30", "R13", "R22", "R31", "R23", "R32", "R33",
)


def exchange_kernel(
    owners, layers, tokens_ref, ids_ref, codes_ref, gate_ref, up_ref, down_ref, out_ref,
    rows, w_gate, w_up, w_down, part_own, part_send, part_recv,
    b_send, b_recv, a_send, a_recv, z_send, z_recv, weight_sem,
    gz_s, gz_r, ga_s, ga_r, gb_s, gb_r, gc_s, gc_r,
    rp_s, rp_r, rb_s, rb_r, ra_s, ra_r, rz_s, rz_r,
):
    tok, half = tokens_ref.shape[1], tokens_ref.shape[2]
    dp, z, core = lax.axis_index("dp"), lax.axis_index("expert"), lax.axis_index("tensor")
    expert = dp * layers + z
    x_peer = dp + 1 - 2 * (dp % 2)
    y_peer = (dp + 2) % 4
    a_peer = {"dp": x_peer * (1 - core) + y_peer * core}
    b_peer = {"dp": y_peer * (1 - core) + x_peer * core}
    c_peer = {"tensor": 1 - core}
    flips = [z, z + 1 - 2 * (z % 2), (z + 2) % 4, 3 - z]
    z_peer = [{"expert": flip} for flip in flips]

    loads = []
    for side in range(2):
        first = pl.multiple_of((core if side == 0 else 1 - core) * half, LANES)
        loads.append(pltpu.make_async_copy(gate_ref.at[0, pl.ds(first, half), :], w_gate.at[side], weight_sem.at[side, 0]))
        loads.append(pltpu.make_async_copy(up_ref.at[0, pl.ds(first, half), :], w_up.at[side], weight_sem.at[side, 1]))
    for side in range(2):
        first = pl.multiple_of((core if side == 0 else 1 - core) * half, LANES)
        loads.append(pltpu.make_async_copy(down_ref.at[0, :, pl.ds(first, half)], w_down.at[side], weight_sem.at[side, 2]))
    for load in loads:
        load.start()

    barrier = pltpu.get_barrier_semaphore()
    peers = [a_peer, b_peer, c_peer] + z_peer[1:]
    for peer in peers:
        pl.semaphore_signal(barrier, inc=1, device_id=peer, device_id_type=MESH)

    rows[0, 0, 0:tok, 0:half] = tokens_ref[0]
    codes = codes_ref[0].astype(jnp.float32)
    share = codes / jnp.sum(codes, axis=1, keepdims=True)
    ids = ids_ref[0]
    lane = lax.broadcasted_iota(jnp.int32, (tok, LANES), 1)
    packed = jnp.zeros((tok, LANES), jnp.float32)
    rest = share
    for term in range(3):
        rounded = rest.astype(jnp.bfloat16).astype(jnp.float32)
        rest = rest - rounded
        for k in range(ids.shape[1]):
            packed = jnp.where(lane == ids[:, k:k + 1] + term * owners, rounded[:, k:k + 1], packed)
    rows[0, 0, 0:tok, half:half + LANES] = packed.astype(jnp.bfloat16)
    pl.semaphore_wait(barrier, len(peers))

    def remote(src, dst, send, recv, peer):
        return pltpu.make_async_remote_copy(
            src_ref=src, dst_ref=dst, send_sem=send, recv_sem=recv, device_id=peer, device_id_type=MESH
        )

    def block(layer, side, spot, count=1, wide=True):
        view = rows.at[layer, side, spot * tok:(spot + count) * tok]
        return view if wide else rows.at[layer, side, spot * tok:(spot + count) * tok, 0:half]

    sent = []

    def send(copy):
        copy.start()
        sent.append(copy)

    gather_z = [None] + [
        remote(block(0, 0, 0), block(i, 0, 0), gz_s.at[i], gz_r.at[i], z_peer[i]) for i in range(1, layers)
    ]
    gather_a = [remote(block(i, 0, 0), block(i, 0, 1), ga_s.at[i], ga_r.at[i], a_peer) for i in range(layers)]
    gather_b = [
        [remote(block(i, 0, s), block(i, 0, 2 + s), gb_s.at[i, s], gb_r.at[i, s], b_peer) for s in range(2)]
        for i in range(layers)
    ]
    swap = (0, 2, 1, 3)
    gather_c = [
        [
            remote(block(i, 0, s, wide=False), block(i, 1, swap[s], wide=False), gc_s.at[i, swap[s]], gc_r.at[i, swap[s]], c_peer)
            for s in range(4)
        ]
        for i in range(layers)
    ]
    reduce_p = [remote(part_send.at[i], part_recv.at[i], rp_s.at[i], rp_r.at[i], c_peer) for i in range(layers)]
    reduce_b = [remote(b_send.at[i], b_recv.at[i], rb_s.at[i], rb_r.at[i], b_peer) for i in range(layers)]
    reduce_a = [remote(a_send.at[i], a_recv.at[i], ra_s.at[i], ra_r.at[i], a_peer) for i in range(layers)]
    reduce_z = [None] + [
        remote(z_send.at[i], z_recv.at[i], rz_s.at[i], rz_r.at[i], z_peer[i]) for i in range(1, layers)
    ]
    kept = [None] * layers
    loaded = []

    def first_hop(i):
        if i == 0:
            for j in range(1, layers):
                send(gather_z[j])
        else:
            gather_z[i].wait_recv()
        send(gather_a[i])
        send(gather_b[i][0])
        send(gather_c[i][0])

    def second_hop(i):
        gather_a[i].wait_recv()
        send(gather_b[i][1])
        send(gather_c[i][1])

    def third_hop(i):
        for s in range(2):
            gather_b[i][s].wait_recv()
            send(gather_c[i][2 + s])

    def compute(i):
        for s in range(4):
            gather_c[i][s].wait_recv()
        if not loaded:
            for load in loads:
                load.wait()
            loaded.append(True)
        own, other = rows[i, 0, :, 0:half], rows[i, 1, :, 0:half]
        dot = functools.partial(jnp.dot, preferred_element_type=jnp.float32)
        gated = dot(own, w_gate[0]) + dot(other, w_gate[1])
        lifted = dot(own, w_up[0]) + dot(other, w_up[1])
        hidden = (gated / (1.0 + jnp.exp(-gated)) * lifted).astype(jnp.bfloat16)
        away = dot(hidden, w_down[1]).astype(jnp.bfloat16)
        for s in range(4):
            part_send[i, swap[s] * tok:(swap[s] + 1) * tok, :] = away[s * tok:(s + 1) * tok]
        send(reduce_p[i])
        part_own[i] = dot(hidden, w_down[0]).astype(jnp.bfloat16)

    def first_sum(i):
        reduce_p[i].wait_recv()
        names = rows[i, 0, :, half:half + LANES].astype(jnp.float32)
        spots = lax.broadcasted_iota(jnp.int32, names.shape, 1)
        mine = (spots == expert) | (spots == expert + owners) | (spots == expert + 2 * owners)
        weight = jnp.sum(jnp.where(mine, names, 0.0), axis=1, keepdims=True)
        total = (part_own[i].astype(jnp.float32) + part_recv[i].astype(jnp.float32)) * weight
        b_send[i] = total[2 * tok:].astype(jnp.bfloat16)
        send(reduce_b[i])
        part_own[i, 0:2 * tok, :] = total[0:2 * tok].astype(jnp.bfloat16)

    def second_sum(i):
        reduce_b[i].wait_recv()
        total = part_own[i, 0:2 * tok, :].astype(jnp.float32) + b_recv[i].astype(jnp.float32)
        a_send[i] = total[tok:].astype(jnp.bfloat16)
        send(reduce_a[i])
        part_own[i, 0:tok, :] = total[0:tok].astype(jnp.bfloat16)

    def third_sum(i):
        reduce_a[i].wait_recv()
        total = part_own[i, 0:tok, :].astype(jnp.float32) + a_recv[i].astype(jnp.float32)
        if i == 0:
            part_own[i, 0:tok, :] = total.astype(jnp.bfloat16)
        else:
            z_send[i] = total.astype(jnp.bfloat16)
            send(reduce_z[i])

    stages = {"F1": first_hop, "F2": second_hop, "F3": third_hop, "R1": first_sum, "R2": second_sum, "R3": third_sum, "C": compute}
    for name in ORDER:
        stages[name[:-1]](int(name[-1]))

    total = part_own[0, 0:tok, :].astype(jnp.float32)
    for i in range(1, layers):
        reduce_z[i].wait_recv()
        total = total + z_recv[i].astype(jnp.float32)
    out_ref[0] = total.astype(out_ref.dtype)
    for copy in sent:
        copy.wait_send()


def exchange(tokens, gate_weight, up_weight, down_weight, expert_ids, gate_codes):
    layers = lax.axis_size("expert")
    owners = lax.axis_size("dp") * layers
    _, tok, half = tokens.shape
    columns = owners // layers
    units = gate_weight.shape[2]
    vmem, hbm = pl.BlockSpec(memory_space=pltpu.VMEM), pl.BlockSpec(memory_space=pl.ANY)
    dma = pltpu.SemaphoreType.DMA
    bf16 = jnp.bfloat16
    pair = (pltpu.VMEM((layers, tok, half), bf16),) * 2
    return pl.pallas_call(
        functools.partial(exchange_kernel, owners, layers),
        out_shape=jax.ShapeDtypeStruct(tokens.shape, tokens.dtype),
        in_specs=[vmem] * 3 + [hbm] * 3,
        out_specs=vmem,
        scratch_shapes=[
            pltpu.VMEM((layers, 2, columns * tok, half + LANES), bf16),
            pltpu.VMEM((2, half, units), bf16),
            pltpu.VMEM((2, half, units), bf16),
            pltpu.VMEM((2, units, half), bf16),
            pltpu.VMEM((layers, columns * tok, half), bf16),
            pltpu.VMEM((layers, columns * tok, half), bf16),
            pltpu.VMEM((layers, columns * tok, half), bf16),
            pltpu.VMEM((layers, 2 * tok, half), bf16),
            pltpu.VMEM((layers, 2 * tok, half), bf16),
            *pair, *pair,
            dma((2, 3)),
            dma((layers,)), dma((layers,)),
            dma((layers,)), dma((layers,)),
            dma((layers, 2)), dma((layers, 2)),
            dma((layers, 4)), dma((layers, 4)),
            *([dma((layers,))] * 8),
        ],
        compiler_params=pltpu.CompilerParams(
            collective_id=0, has_side_effects=True, vmem_limit_bytes=48 * 1024 * 1024
        ),
    )(tokens, expert_ids, gate_codes, gate_weight, up_weight, down_weight)


def local(tokens, gate_weight, up_weight, down_weight, expert_ids, gate_codes):
    owners = lax.axis_size("dp") * lax.axis_size("expert")
    tok_rows = tokens.shape[1]
    top_count = expert_ids.shape[2]
    slot_depth = min(tok_rows, max(2, 2 * tok_rows * top_count // owners))
    if (
        slot_depth == tok_rows and lax.axis_size("dp") == 4 and lax.axis_size("expert") == 4
        and lax.axis_size("tensor") == 2 and tokens.shape[0] == 1 and tok_rows % 16 == 0
    ):
        return exchange(tokens, gate_weight, up_weight, down_weight, expert_ids, gate_codes)
    slot_count = owners * slot_depth
    w_gate = gate_weight[0]
    w_up = up_weight[0]
    w_down = down_weight[0]
    slot_numbers = jnp.arange(slot_count, dtype=jnp.int32)
    owner_numbers = jnp.arange(owners, dtype=jnp.int32)
    step_tokens = tokens[0]
    route_ids = expert_ids[0].reshape(tok_rows * top_count)
    onehot = (route_ids[:, None] == owner_numbers[None, :]).astype(jnp.int32)
    before = jnp.cumsum(onehot, axis=0) - onehot
    slot_rank = jnp.sum(before * onehot, axis=1)
    slot_index = route_ids * slot_depth + slot_rank
    select = (slot_index[:, None] == slot_numbers[None, :]).astype(jnp.bfloat16)
    per_token = jnp.sum(select.reshape(tok_rows, top_count, slot_count), axis=1)
    packed = jnp.einsum(
        "ts,td->sd", per_token, step_tokens, preferred_element_type=jnp.float32
    ).astype(jnp.bfloat16)
    packed = packed.reshape(owners, slot_depth, step_tokens.shape[1])
    arrived = lax.all_to_all(packed, ("dp", "expert"), split_axis=0, concat_axis=0, tiled=True)
    owner_rows = arrived.reshape(slot_count, step_tokens.shape[1])
    owner_rows = lax.all_gather(owner_rows, "tensor", axis=1, tiled=True)
    gated = jnp.dot(owner_rows, w_gate, preferred_element_type=jnp.float32)
    lifted = jnp.dot(owner_rows, w_up, preferred_element_type=jnp.float32)
    hidden = (jax.nn.silu(gated) * lifted).astype(jnp.bfloat16)
    partial_value = jnp.dot(hidden, w_down, preferred_element_type=jnp.float32).astype(jnp.bfloat16)
    summed = (
        lax.psum_scatter(partial_value, "tensor", scatter_dimension=1, tiled=True)
        .astype(jnp.float32)
        .astype(jnp.bfloat16)
    )
    half_width = summed.shape[1]
    result = summed.reshape(owners, slot_depth, half_width)
    returned = lax.all_to_all(result, ("dp", "expert"), split_axis=0, concat_axis=0, tiled=True)
    returned = returned.reshape(slot_count, half_width)
    picked = jnp.dot(select, returned, preferred_element_type=jnp.float32)
    codes = gate_codes[0].astype(jnp.float32)
    shares = codes / jnp.sum(codes, axis=1, keepdims=True)
    mixed_rows = jnp.sum(
        picked.reshape(tok_rows, top_count, half_width) * shares[:, :, None], axis=1
    )
    outputs = [mixed_rows.astype(jnp.bfloat16)]
    return jnp.stack(outputs)


def solution(mesh):
    in_specs = (
        P(None, ("dp", "expert"), "tensor"),
        P(("dp", "expert"), None, "tensor"),
        P(("dp", "expert"), None, "tensor"),
        P(("dp", "expert"), "tensor", None),
        P(None, ("dp", "expert"), None),
        P(None, ("dp", "expert"), None),
    )
    out_specs = P(None, ("dp", "expert"), "tensor")
    return jax.shard_map(local, mesh=mesh, in_specs=in_specs, out_specs=out_specs, check_vma=False)
```

```python
import functools
import jax
import jax.numpy as jnp
from jax import lax
from jax.experimental import pallas as pl
from jax.experimental.pallas import tpu as pltpu
from jax.sharding import PartitionSpec as P

MESH = pl.DeviceIdType.MESH
LANES = 128
ORDER = (
    "F10", "F11", "F20", "F12", "F21", "F30", "F13", "F22", "F31", "C0", "F23", "F32", "C1", "R10",
    "F33", "C2", "R11", "R20", "C3", "R12", "R21", "R30", "R13", "R22", "R31", "R23", "R32", "R33",
)


def exchange_kernel(
    owners, layers, tokens_ref, ids_ref, codes_ref, gate_ref, up_ref, down_ref, out_ref,
    rows, w_gate, w_up, w_down, part_own, part_send, part_recv,
    b_send, b_recv, a_send, a_recv, z_send, z_recv, weight_sem,
    gz_s, gz_r, ga_s, ga_r, gb_s, gb_r, gc_s, gc_r,
    rp_s, rp_r, rb_s, rb_r, ra_s, ra_r, rz_s, rz_r,
):
    tok, half = tokens_ref.shape[1], tokens_ref.shape[2]
    dp, z, core = lax.axis_index("dp"), lax.axis_index("expert"), lax.axis_index("tensor")
    expert = dp * layers + z
    x_peer = dp + 1 - 2 * (dp % 2)
    y_peer = (dp + 2) % 4
    a_peer = {"dp": x_peer * (1 - core) + y_peer * core}
    b_peer = {"dp": y_peer * (1 - core) + x_peer * core}
    c_peer = {"tensor": 1 - core}
    flips = [z, z + 1 - 2 * (z % 2), (z + 2) % 4, 3 - z]
    z_peer = [{"expert": flip} for flip in flips]

    loads = []
    for side in range(2):
        first = pl.multiple_of((core if side == 0 else 1 - core) * half, LANES)
        loads.append(pltpu.make_async_copy(gate_ref.at[0, pl.ds(first, half), :], w_gate.at[side], weight_sem.at[side, 0]))
        loads.append(pltpu.make_async_copy(up_ref.at[0, pl.ds(first, half), :], w_up.at[side], weight_sem.at[side, 1]))
    for side in range(2):
        first = pl.multiple_of((core if side == 0 else 1 - core) * half, LANES)
        loads.append(pltpu.make_async_copy(down_ref.at[0, :, pl.ds(first, half)], w_down.at[side], weight_sem.at[side, 2]))
    for load in loads:
        load.start()

    barrier = pltpu.get_barrier_semaphore()
    peers = [a_peer, b_peer, c_peer] + z_peer[1:]
    for peer in peers:
        pl.semaphore_signal(barrier, inc=1, device_id=peer, device_id_type=MESH)

    rows[0, 0, 0:tok, 0:half] = tokens_ref[0]
    codes = codes_ref[0].astype(jnp.float32).T
    share = codes / jnp.sum(codes, axis=1, keepdims=True)
    ids = ids_ref[0].T
    lane = lax.broadcasted_iota(jnp.int32, (tok, LANES), 1)
    packed = jnp.zeros((tok, LANES), jnp.float32)
    rest = share
    for term in range(3):
        rounded = rest.astype(jnp.bfloat16).astype(jnp.float32)
        rest = rest - rounded
        for k in range(ids.shape[1]):
            packed = jnp.where(lane == ids[:, k:k + 1] + term * owners, rounded[:, k:k + 1], packed)
    rows[0, 0, 0:tok, half:half + LANES] = packed.astype(jnp.bfloat16)
    pl.semaphore_wait(barrier, len(peers))

    def remote(src, dst, send, recv, peer):
        return pltpu.make_async_remote_copy(
            src_ref=src, dst_ref=dst, send_sem=send, recv_sem=recv, device_id=peer, device_id_type=MESH
        )

    def block(layer, side, spot, count=1, wide=True):
        view = rows.at[layer, side, spot * tok:(spot + count) * tok]
        return view if wide else rows.at[layer, side, spot * tok:(spot + count) * tok, 0:half]

    sent = []

    def send(copy):
        copy.start()
        sent.append(copy)

    gather_z = [None] + [
        remote(block(0, 0, 0), block(i, 0, 0), gz_s.at[i], gz_r.at[i], z_peer[i]) for i in range(1, layers)
    ]
    gather_a = [remote(block(i, 0, 0), block(i, 0, 1), ga_s.at[i], ga_r.at[i], a_peer) for i in range(layers)]
    gather_b = [
        [remote(block(i, 0, s), block(i, 0, 2 + s), gb_s.at[i, s], gb_r.at[i, s], b_peer) for s in range(2)]
        for i in range(layers)
    ]
    swap = (0, 2, 1, 3)
    gather_c = [
        [
            remote(block(i, 0, s, wide=False), block(i, 1, swap[s], wide=False), gc_s.at[i, swap[s]], gc_r.at[i, swap[s]], c_peer)
            for s in range(4)
        ]
        for i in range(layers)
    ]
    reduce_p = [remote(part_send.at[i], part_recv.at[i], rp_s.at[i], rp_r.at[i], c_peer) for i in range(layers)]
    reduce_b = [remote(b_send.at[i], b_recv.at[i], rb_s.at[i], rb_r.at[i], b_peer) for i in range(layers)]
    reduce_a = [remote(a_send.at[i], a_recv.at[i], ra_s.at[i], ra_r.at[i], a_peer) for i in range(layers)]
    reduce_z = [None] + [
        remote(z_send.at[i], z_recv.at[i], rz_s.at[i], rz_r.at[i], z_peer[i]) for i in range(1, layers)
    ]
    kept = [None] * layers
    loaded = []

    def first_hop(i):
        if i == 0:
            for j in range(1, layers):
                send(gather_z[j])
        else:
            gather_z[i].wait_recv()
        send(gather_a[i])
        send(gather_b[i][0])
        send(gather_c[i][0])

    def second_hop(i):
        gather_a[i].wait_recv()
        send(gather_b[i][1])
        send(gather_c[i][1])

    def third_hop(i):
        for s in range(2):
            gather_b[i][s].wait_recv()
            send(gather_c[i][2 + s])

    def compute(i):
        for s in range(4):
            gather_c[i][s].wait_recv()
        if not loaded:
            for load in loads:
                load.wait()
            loaded.append(True)
        own, other = rows[i, 0, :, 0:half], rows[i, 1, :, 0:half]
        dot = functools.partial(jnp.dot, preferred_element_type=jnp.float32)
        gated = dot(own, w_gate[0]) + dot(other, w_gate[1])
        lifted = dot(own, w_up[0]) + dot(other, w_up[1])
        hidden = (gated / (1.0 + jnp.exp(-gated)) * lifted).astype(jnp.bfloat16)
        away = dot(hidden, w_down[1]).astype(jnp.bfloat16)
        for s in range(4):
            part_send[i, swap[s] * tok:(swap[s] + 1) * tok, :] = away[s * tok:(s + 1) * tok]
        send(reduce_p[i])
        part_own[i] = dot(hidden, w_down[0]).astype(jnp.bfloat16)

    def first_sum(i):
        reduce_p[i].wait_recv()
        names = rows[i, 0, :, half:half + LANES].astype(jnp.float32)
        spots = lax.broadcasted_iota(jnp.int32, names.shape, 1)
        mine = (spots == expert) | (spots == expert + owners) | (spots == expert + 2 * owners)
        weight = jnp.sum(jnp.where(mine, names, 0.0), axis=1, keepdims=True)
        total = (part_own[i].astype(jnp.float32) + part_recv[i].astype(jnp.float32)) * weight
        b_send[i] = total[2 * tok:].astype(jnp.bfloat16)
        send(reduce_b[i])
        part_own[i, 0:2 * tok, :] = total[0:2 * tok].astype(jnp.bfloat16)

    def second_sum(i):
        reduce_b[i].wait_recv()
        total = part_own[i, 0:2 * tok, :].astype(jnp.float32) + b_recv[i].astype(jnp.float32)
        a_send[i] = total[tok:].astype(jnp.bfloat16)
        send(reduce_a[i])
        part_own[i, 0:tok, :] = total[0:tok].astype(jnp.bfloat16)

    def third_sum(i):
        reduce_a[i].wait_recv()
        total = part_own[i, 0:tok, :].astype(jnp.float32) + a_recv[i].astype(jnp.float32)
        if i == 0:
            part_own[i, 0:tok, :] = total.astype(jnp.bfloat16)
        else:
            z_send[i] = total.astype(jnp.bfloat16)
            send(reduce_z[i])

    stages = {"F1": first_hop, "F2": second_hop, "F3": third_hop, "R1": first_sum, "R2": second_sum, "R3": third_sum, "C": compute}
    for name in ORDER:
        stages[name[:-1]](int(name[-1]))

    total = part_own[0, 0:tok, :].astype(jnp.float32)
    for i in range(1, layers):
        reduce_z[i].wait_recv()
        total = total + z_recv[i].astype(jnp.float32)
    out_ref[0] = total.astype(out_ref.dtype)
    for copy in sent:
        copy.wait_send()


def exchange(tokens, gate_weight, up_weight, down_weight, expert_ids, gate_codes):
    layers = lax.axis_size("expert")
    owners = lax.axis_size("dp") * layers
    _, tok, half = tokens.shape
    columns = owners // layers
    units = gate_weight.shape[2]
    vmem, hbm = pl.BlockSpec(memory_space=pltpu.VMEM), pl.BlockSpec(memory_space=pl.ANY)
    dma = pltpu.SemaphoreType.DMA
    bf16 = jnp.bfloat16
    pair = (pltpu.VMEM((layers, tok, half), bf16),) * 2
    return pl.pallas_call(
        functools.partial(exchange_kernel, owners, layers),
        out_shape=jax.ShapeDtypeStruct(tokens.shape, tokens.dtype),
        in_specs=[vmem] * 3 + [hbm] * 3,
        out_specs=vmem,
        scratch_shapes=[
            pltpu.VMEM((layers, 2, columns * tok, half + LANES), bf16),
            pltpu.VMEM((2, half, units), bf16),
            pltpu.VMEM((2, half, units), bf16),
            pltpu.VMEM((2, units, half), bf16),
            pltpu.VMEM((layers, columns * tok, half), bf16),
            pltpu.VMEM((layers, columns * tok, half), bf16),
            pltpu.VMEM((layers, columns * tok, half), bf16),
            pltpu.VMEM((layers, 2 * tok, half), bf16),
            pltpu.VMEM((layers, 2 * tok, half), bf16),
            *pair, *pair,
            dma((2, 3)),
            dma((layers,)), dma((layers,)),
            dma((layers,)), dma((layers,)),
            dma((layers, 2)), dma((layers, 2)),
            dma((layers, 4)), dma((layers, 4)),
            *([dma((layers,))] * 8),
        ],
        compiler_params=pltpu.CompilerParams(
            collective_id=0, has_side_effects=True, vmem_limit_bytes=63 * 1024 * 1024
        ),
    )(tokens, expert_ids.swapaxes(1, 2), gate_codes.swapaxes(1, 2), gate_weight, up_weight, down_weight)


def local(tokens, gate_weight, up_weight, down_weight, expert_ids, gate_codes):
    owners = lax.axis_size("dp") * lax.axis_size("expert")
    tok_rows = tokens.shape[1]
    top_count = expert_ids.shape[2]
    slot_depth = min(tok_rows, max(2, 2 * tok_rows * top_count // owners))
    if (
        slot_depth == tok_rows and lax.axis_size("dp") == 4 and lax.axis_size("expert") == 4
        and lax.axis_size("tensor") == 2 and tokens.shape[0] == 1 and tok_rows % 16 == 0
    ):
        return exchange(tokens, gate_weight, up_weight, down_weight, expert_ids, gate_codes)
    slot_count = owners * slot_depth
    w_gate = gate_weight[0]
    w_up = up_weight[0]
    w_down = down_weight[0]
    slot_numbers = jnp.arange(slot_count, dtype=jnp.int32)
    owner_numbers = jnp.arange(owners, dtype=jnp.int32)
    step_tokens = tokens[0]
    route_ids = expert_ids[0].reshape(tok_rows * top_count)
    onehot = (route_ids[:, None] == owner_numbers[None, :]).astype(jnp.int32)
    before = jnp.cumsum(onehot, axis=0) - onehot
    slot_rank = jnp.sum(before * onehot, axis=1)
    slot_index = route_ids * slot_depth + slot_rank
    select = (slot_index[:, None] == slot_numbers[None, :]).astype(jnp.bfloat16)
    per_token = jnp.sum(select.reshape(tok_rows, top_count, slot_count), axis=1)
    packed = jnp.einsum(
        "ts,td->sd", per_token, step_tokens, preferred_element_type=jnp.float32
    ).astype(jnp.bfloat16)
    packed = packed.reshape(owners, slot_depth, step_tokens.shape[1])
    arrived = lax.all_to_all(packed, ("dp", "expert"), split_axis=0, concat_axis=0, tiled=True)
    owner_rows = arrived.reshape(slot_count, step_tokens.shape[1])
    owner_rows = lax.all_gather(owner_rows, "tensor", axis=1, tiled=True)
    gated = jnp.dot(owner_rows, w_gate, preferred_element_type=jnp.float32)
    lifted = jnp.dot(owner_rows, w_up, preferred_element_type=jnp.float32)
    hidden = (jax.nn.silu(gated) * lifted).astype(jnp.bfloat16)
    partial_value = jnp.dot(hidden, w_down, preferred_element_type=jnp.float32).astype(jnp.bfloat16)
    summed = (
        lax.psum_scatter(partial_value, "tensor", scatter_dimension=1, tiled=True)
        .astype(jnp.float32)
        .astype(jnp.bfloat16)
    )
    half_width = summed.shape[1]
    result = summed.reshape(owners, slot_depth, half_width)
    returned = lax.all_to_all(result, ("dp", "expert"), split_axis=0, concat_axis=0, tiled=True)
    returned = returned.reshape(slot_count, half_width)
    picked = jnp.dot(select, returned, preferred_element_type=jnp.float32)
    codes = gate_codes[0].astype(jnp.float32)
    shares = codes / jnp.sum(codes, axis=1, keepdims=True)
    mixed_rows = jnp.sum(
        picked.reshape(tok_rows, top_count, half_width) * shares[:, :, None], axis=1
    )
    outputs = [mixed_rows.astype(jnp.bfloat16)]
    return jnp.stack(outputs)


def solution(mesh):
    in_specs = (
        P(None, ("dp", "expert"), "tensor"),
        P(("dp", "expert"), None, "tensor"),
        P(("dp", "expert"), None, "tensor"),
        P(("dp", "expert"), "tensor", None),
        P(None, ("dp", "expert"), None),
        P(None, ("dp", "expert"), None),
    )
    out_specs = P(None, ("dp", "expert"), "tensor")
    return jax.shard_map(local, mesh=mesh, in_specs=in_specs, out_specs=out_specs, check_vma=False)
```

```python
import functools
import jax
import jax.numpy as jnp
from jax import lax
from jax.experimental import pallas as pl
from jax.experimental.pallas import tpu as pltpu
from jax.sharding import PartitionSpec as P

MESH = pl.DeviceIdType.MESH
LANES = 128
ORDER = ("F10", "F11", "F20", "F12", "F21", "F30", "F13", "F22", "F31", "F23", "F32", "C0", "F33", "R10", "R11", "C1", "R20", "R21", "R12", "R13", "R30", "R31", "R22", "R23", "R32", "R33",)


def exchange_kernel(
    owners, layers, tokens_ref, ids_ref, codes_ref, gate_ref, up_ref, down_ref, out_ref,
    rows, w_gate, w_up, w_down, part_own, part_send, part_recv,
    b_send, b_recv, a_send, a_recv, z_send, z_recv, weight_sem,
    gz_s, gz_r, ga_s, ga_r, gb_s, gb_r, gc_s, gc_r,
    rp_s, rp_r, rb_s, rb_r, ra_s, ra_r, rz_s, rz_r,
):
    tok, half = tokens_ref.shape[1], tokens_ref.shape[2]
    dp, z, core = lax.axis_index("dp"), lax.axis_index("expert"), lax.axis_index("tensor")
    expert = dp * layers + z
    x_peer = dp + 1 - 2 * (dp % 2)
    y_peer = (dp + 2) % 4
    a_peer = {"dp": x_peer * (1 - core) + y_peer * core}
    b_peer = {"dp": y_peer * (1 - core) + x_peer * core}
    c_peer = {"tensor": 1 - core}
    flips = [z, z + 1 - 2 * (z % 2), (z + 2) % 4, 3 - z]
    z_peer = [{"expert": flip} for flip in flips]

    loads = []
    for side in range(2):
        first = pl.multiple_of((core if side == 0 else 1 - core) * half, LANES)
        loads.append(pltpu.make_async_copy(gate_ref.at[0, pl.ds(first, half), :], w_gate.at[side], weight_sem.at[side, 0]))
        loads.append(pltpu.make_async_copy(up_ref.at[0, pl.ds(first, half), :], w_up.at[side], weight_sem.at[side, 1]))
    for side in range(2):
        first = pl.multiple_of((core if side == 0 else 1 - core) * half, LANES)
        loads.append(pltpu.make_async_copy(down_ref.at[0, :, pl.ds(first, half)], w_down.at[side], weight_sem.at[side, 2]))
    for load in loads:
        load.start()

    barrier = pltpu.get_barrier_semaphore()
    peers = [a_peer, b_peer, c_peer] + z_peer[1:]
    for peer in peers:
        pl.semaphore_signal(barrier, inc=1, device_id=peer, device_id_type=MESH)

    rows[0, 0, 0:tok, 0:half] = tokens_ref[0]
    codes = codes_ref[0].astype(jnp.float32).T
    share = codes / jnp.sum(codes, axis=1, keepdims=True)
    ids = ids_ref[0].T
    lane = lax.broadcasted_iota(jnp.int32, (tok, LANES), 1)
    packed = jnp.zeros((tok, LANES), jnp.float32)
    rest = share
    for term in range(3):
        rounded = rest.astype(jnp.bfloat16).astype(jnp.float32)
        rest = rest - rounded
        for k in range(ids.shape[1]):
            packed = jnp.where(lane == ids[:, k:k + 1] + term * owners, rounded[:, k:k + 1], packed)
    rows[0, 0, 0:tok, half:half + LANES] = packed.astype(jnp.bfloat16)
    pl.semaphore_wait(barrier, len(peers))

    def remote(src, dst, send, recv, peer):
        return pltpu.make_async_remote_copy(
            src_ref=src, dst_ref=dst, send_sem=send, recv_sem=recv, device_id=peer, device_id_type=MESH
        )

    def block(layer, side, spot, count=1, wide=True):
        view = rows.at[layer, side, spot * tok:(spot + count) * tok]
        return view if wide else rows.at[layer, side, spot * tok:(spot + count) * tok, 0:half]

    sent = []

    def send(copy):
        copy.start()
        sent.append(copy)

    gather_z = [None] + [
        remote(block(0, 0, 0), block(i, 0, 0), gz_s.at[i], gz_r.at[i], z_peer[i]) for i in range(1, layers)
    ]
    gather_a = [remote(block(i, 0, 0), block(i, 0, 1), ga_s.at[i], ga_r.at[i], a_peer) for i in range(layers)]
    gather_b = [
        [remote(block(i, 0, s), block(i, 0, 2 + s), gb_s.at[i, s], gb_r.at[i, s], b_peer) for s in range(2)]
        for i in range(layers)
    ]
    swap = (0, 2, 1, 3)
    gather_c = [
        [
            remote(block(i, 0, s, wide=False), block(i, 1, swap[s], wide=False), gc_s.at[i, swap[s]], gc_r.at[i, swap[s]], c_peer)
            for s in range(4)
        ]
        for i in range(layers)
    ]
    reduce_p = [remote(part_send.at[i], part_recv.at[i], rp_s.at[i], rp_r.at[i], c_peer) for i in range(layers)]
    reduce_b = [remote(b_send.at[i], b_recv.at[i], rb_s.at[i], rb_r.at[i], b_peer) for i in range(layers)]
    reduce_a = [remote(a_send.at[i], a_recv.at[i], ra_s.at[i], ra_r.at[i], a_peer) for i in range(layers)]
    reduce_z = [None] + [
        remote(z_send.at[i], z_recv.at[i], rz_s.at[i], rz_r.at[i], z_peer[i]) for i in range(1, layers)
    ]
    kept = [None] * layers
    loaded = []

    def first_hop(i):
        if i == 0:
            for j in range(1, layers):
                send(gather_z[j])
        else:
            gather_z[i].wait_recv()
        send(gather_a[i])
        send(gather_b[i][0])
        send(gather_c[i][0])

    def second_hop(i):
        gather_a[i].wait_recv()
        send(gather_b[i][1])
        send(gather_c[i][1])

    def third_hop(i):
        for s in range(2):
            gather_b[i][s].wait_recv()
            send(gather_c[i][2 + s])

    def compute(j):
        pair = (2 * j, 2 * j + 1)
        for i in pair:
            for s in range(4):
                gather_c[i][s].wait_recv()
        if not loaded:
            for load in loads:
                load.wait()
            loaded.append(True)
        count = 4 * tok
        own = rows[2 * j:2 * j + 2, 0, :, 0:half].reshape(2 * count, half)
        other = rows[2 * j:2 * j + 2, 1, :, 0:half].reshape(2 * count, half)
        dot = functools.partial(jnp.dot, preferred_element_type=jnp.float32)
        gated = dot(own, w_gate[0]) + dot(other, w_gate[1])
        lifted = dot(own, w_up[0]) + dot(other, w_up[1])
        hidden = (gated / (1.0 + jnp.exp(-gated)) * lifted).astype(jnp.bfloat16)
        away = dot(hidden, w_down[1]).astype(jnp.bfloat16)
        for i in pair:
            for s in range(4):
                first = (i % 2) * count + s * tok
                part_send[i, swap[s] * tok:(swap[s] + 1) * tok, :] = away[first:first + tok]
            send(reduce_p[i])
        part_own[2 * j:2 * j + 2] = dot(hidden, w_down[0]).astype(jnp.bfloat16).reshape(2, count, half)

    def first_sum(i):
        reduce_p[i].wait_recv()
        names = rows[i, 0, :, half:half + LANES].astype(jnp.float32)
        spots = lax.broadcasted_iota(jnp.int32, names.shape, 1)
        mine = (spots == expert) | (spots == expert + owners) | (spots == expert + 2 * owners)
        weight = jnp.sum(jnp.where(mine, names, 0.0), axis=1, keepdims=True)
        total = (part_own[i].astype(jnp.float32) + part_recv[i].astype(jnp.float32)) * weight
        b_send[i] = total[2 * tok:].astype(jnp.bfloat16)
        send(reduce_b[i])
        part_own[i, 0:2 * tok, :] = total[0:2 * tok].astype(jnp.bfloat16)

    def second_sum(i):
        reduce_b[i].wait_recv()
        total = part_own[i, 0:2 * tok, :].astype(jnp.float32) + b_recv[i].astype(jnp.float32)
        a_send[i] = total[tok:].astype(jnp.bfloat16)
        send(reduce_a[i])
        part_own[i, 0:tok, :] = total[0:tok].astype(jnp.bfloat16)

    def third_sum(i):
        reduce_a[i].wait_recv()
        total = part_own[i, 0:tok, :].astype(jnp.float32) + a_recv[i].astype(jnp.float32)
        if i == 0:
            part_own[i, 0:tok, :] = total.astype(jnp.bfloat16)
        else:
            z_send[i] = total.astype(jnp.bfloat16)
            send(reduce_z[i])

    stages = {"F1": first_hop, "F2": second_hop, "F3": third_hop, "R1": first_sum, "R2": second_sum, "R3": third_sum, "C": compute}
    for name in ORDER:
        stages[name[:-1]](int(name[-1]))

    total = part_own[0, 0:tok, :].astype(jnp.float32)
    for i in range(1, layers):
        reduce_z[i].wait_recv()
        total = total + z_recv[i].astype(jnp.float32)
    out_ref[0] = total.astype(out_ref.dtype)
    for copy in sent:
        copy.wait_send()


def exchange(tokens, gate_weight, up_weight, down_weight, expert_ids, gate_codes):
    layers = lax.axis_size("expert")
    owners = lax.axis_size("dp") * layers
    _, tok, half = tokens.shape
    columns = owners // layers
    units = gate_weight.shape[2]
    vmem, hbm = pl.BlockSpec(memory_space=pltpu.VMEM), pl.BlockSpec(memory_space=pl.ANY)
    dma = pltpu.SemaphoreType.DMA
    bf16 = jnp.bfloat16
    pair = (pltpu.VMEM((layers, tok, half), bf16),) * 2
    return pl.pallas_call(
        functools.partial(exchange_kernel, owners, layers),
        out_shape=jax.ShapeDtypeStruct(tokens.shape, tokens.dtype),
        in_specs=[vmem] * 3 + [hbm] * 3,
        out_specs=vmem,
        scratch_shapes=[
            pltpu.VMEM((layers, 2, columns * tok, half + LANES), bf16),
            pltpu.VMEM((2, half, units), bf16),
            pltpu.VMEM((2, half, units), bf16),
            pltpu.VMEM((2, units, half), bf16),
            pltpu.VMEM((layers, columns * tok, half), bf16),
            pltpu.VMEM((layers, columns * tok, half), bf16),
            pltpu.VMEM((layers, columns * tok, half), bf16),
            pltpu.VMEM((layers, 2 * tok, half), bf16),
            pltpu.VMEM((layers, 2 * tok, half), bf16),
            *pair, *pair,
            dma((2, 3)),
            dma((layers,)), dma((layers,)),
            dma((layers,)), dma((layers,)),
            dma((layers, 2)), dma((layers, 2)),
            dma((layers, 4)), dma((layers, 4)),
            *([dma((layers,))] * 8),
        ],
        compiler_params=pltpu.CompilerParams(
            collective_id=0, has_side_effects=True, vmem_limit_bytes=63 * 1024 * 1024
        ),
    )(tokens, expert_ids.swapaxes(1, 2), gate_codes.swapaxes(1, 2), gate_weight, up_weight, down_weight)


def local(tokens, gate_weight, up_weight, down_weight, expert_ids, gate_codes):
    owners = lax.axis_size("dp") * lax.axis_size("expert")
    tok_rows = tokens.shape[1]
    top_count = expert_ids.shape[2]
    slot_depth = min(tok_rows, max(2, 2 * tok_rows * top_count // owners))
    if (
        slot_depth == tok_rows and lax.axis_size("dp") == 4 and lax.axis_size("expert") == 4
        and lax.axis_size("tensor") == 2 and tokens.shape[0] == 1 and tok_rows % 16 == 0
    ):
        return exchange(tokens, gate_weight, up_weight, down_weight, expert_ids, gate_codes)
    slot_count = owners * slot_depth
    w_gate = gate_weight[0]
    w_up = up_weight[0]
    w_down = down_weight[0]
    slot_numbers = jnp.arange(slot_count, dtype=jnp.int32)
    owner_numbers = jnp.arange(owners, dtype=jnp.int32)
    step_tokens = tokens[0]
    route_ids = expert_ids[0].reshape(tok_rows * top_count)
    onehot = (route_ids[:, None] == owner_numbers[None, :]).astype(jnp.int32)
    before = jnp.cumsum(onehot, axis=0) - onehot
    slot_rank = jnp.sum(before * onehot, axis=1)
    slot_index = route_ids * slot_depth + slot_rank
    select = (slot_index[:, None] == slot_numbers[None, :]).astype(jnp.bfloat16)
    per_token = jnp.sum(select.reshape(tok_rows, top_count, slot_count), axis=1)
    packed = jnp.einsum(
        "ts,td->sd", per_token, step_tokens, preferred_element_type=jnp.float32
    ).astype(jnp.bfloat16)
    packed = packed.reshape(owners, slot_depth, step_tokens.shape[1])
    arrived = lax.all_to_all(packed, ("dp", "expert"), split_axis=0, concat_axis=0, tiled=True)
    owner_rows = arrived.reshape(slot_count, step_tokens.shape[1])
    owner_rows = lax.all_gather(owner_rows, "tensor", axis=1, tiled=True)
    gated = jnp.dot(owner_rows, w_gate, preferred_element_type=jnp.float32)
    lifted = jnp.dot(owner_rows, w_up, preferred_element_type=jnp.float32)
    hidden = (jax.nn.silu(gated) * lifted).astype(jnp.bfloat16)
    partial_value = jnp.dot(hidden, w_down, preferred_element_type=jnp.float32).astype(jnp.bfloat16)
    summed = (
        lax.psum_scatter(partial_value, "tensor", scatter_dimension=1, tiled=True)
        .astype(jnp.float32)
        .astype(jnp.bfloat16)
    )
    half_width = summed.shape[1]
    result = summed.reshape(owners, slot_depth, half_width)
    returned = lax.all_to_all(result, ("dp", "expert"), split_axis=0, concat_axis=0, tiled=True)
    returned = returned.reshape(slot_count, half_width)
    picked = jnp.dot(select, returned, preferred_element_type=jnp.float32)
    codes = gate_codes[0].astype(jnp.float32)
    shares = codes / jnp.sum(codes, axis=1, keepdims=True)
    mixed_rows = jnp.sum(
        picked.reshape(tok_rows, top_count, half_width) * shares[:, :, None], axis=1
    )
    outputs = [mixed_rows.astype(jnp.bfloat16)]
    return jnp.stack(outputs)


def solution(mesh):
    in_specs = (
        P(None, ("dp", "expert"), "tensor"),
        P(("dp", "expert"), None, "tensor"),
        P(("dp", "expert"), None, "tensor"),
        P(("dp", "expert"), "tensor", None),
        P(None, ("dp", "expert"), None),
        P(None, ("dp", "expert"), None),
    )
    out_specs = P(None, ("dp", "expert"), "tensor")
    return jax.shard_map(local, mesh=mesh, in_specs=in_specs, out_specs=out_specs, check_vma=False)
```

```python
import functools
import jax
import jax.numpy as jnp
from jax import lax
from jax.experimental import pallas as pl
from jax.experimental.pallas import tpu as pltpu
from jax.sharding import PartitionSpec as P

MESH = pl.DeviceIdType.MESH
LANES = 128
ORDER = ("F10", "F11", "F20", "F12", "F21", "F30", "F13", "F22", "F31", "F23", "C0", "F32", "F33", "R11", "R10", "C1", "R12", "R13", "R21", "R20", "R22", "R23", "R31", "R32", "R33", "R30",)


def exchange_kernel(
    owners, layers, tokens_ref, ids_ref, codes_ref, gate_ref, up_ref, down_ref, out_ref,
    rows, w_gate, w_up, w_down, part_own, part_send, part_recv,
    b_send, b_recv, a_send, a_recv, z_send, z_recv, weight_sem,
    gz_s, gz_r, ga_s, ga_r, gb_s, gb_r, gc_s, gc_r,
    rp_s, rp_r, rb_s, rb_r, ra_s, ra_r, rz_s, rz_r,
):
    tok, half = tokens_ref.shape[1], tokens_ref.shape[2]
    dp, z, core = lax.axis_index("dp"), lax.axis_index("expert"), lax.axis_index("tensor")
    expert = dp * layers + z
    x_peer = dp + 1 - 2 * (dp % 2)
    y_peer = (dp + 2) % 4
    a_peer = {"dp": x_peer * (1 - core) + y_peer * core}
    b_peer = {"dp": y_peer * (1 - core) + x_peer * core}
    c_peer = {"tensor": 1 - core}
    flips = [z, z + 1 - 2 * (z % 2), (z + 2) % 4, 3 - z]
    z_peer = [{"expert": flip} for flip in flips]

    loads = []
    for side in range(2):
        first = pl.multiple_of((core if side == 0 else 1 - core) * half, LANES)
        loads.append(pltpu.make_async_copy(gate_ref.at[0, pl.ds(first, half), :], w_gate.at[side], weight_sem.at[side, 0]))
        loads.append(pltpu.make_async_copy(up_ref.at[0, pl.ds(first, half), :], w_up.at[side], weight_sem.at[side, 1]))
    for side in range(2):
        first = pl.multiple_of((core if side == 0 else 1 - core) * half, LANES)
        loads.append(pltpu.make_async_copy(down_ref.at[0, :, pl.ds(first, half)], w_down.at[side], weight_sem.at[side, 2]))
    for load in loads:
        load.start()

    barrier = pltpu.get_barrier_semaphore()
    peers = [a_peer, b_peer, c_peer] + z_peer[1:]
    for peer in peers:
        pl.semaphore_signal(barrier, inc=1, device_id=peer, device_id_type=MESH)

    rows[0, 0, 0:tok, 0:half] = tokens_ref[0]
    codes = codes_ref[0].astype(jnp.float32).T
    share = codes / jnp.sum(codes, axis=1, keepdims=True)
    ids = ids_ref[0].T
    lane = lax.broadcasted_iota(jnp.int32, (tok, LANES), 1)
    packed = jnp.zeros((tok, LANES), jnp.float32)
    rest = share
    for term in range(3):
        rounded = rest.astype(jnp.bfloat16).astype(jnp.float32)
        rest = rest - rounded
        for k in range(ids.shape[1]):
            packed = jnp.where(lane == ids[:, k:k + 1] + term * owners, rounded[:, k:k + 1], packed)
    rows[0, 0, 0:tok, half:half + LANES] = packed.astype(jnp.bfloat16)
    pl.semaphore_wait(barrier, len(peers))

    def remote(src, dst, send, recv, peer):
        return pltpu.make_async_remote_copy(
            src_ref=src, dst_ref=dst, send_sem=send, recv_sem=recv, device_id=peer, device_id_type=MESH
        )

    def block(layer, side, spot, count=1, wide=True):
        view = rows.at[layer, side, spot * tok:(spot + count) * tok]
        return view if wide else rows.at[layer, side, spot * tok:(spot + count) * tok, 0:half]

    sent = []

    def send(copy):
        copy.start()
        sent.append(copy)

    gather_z = [None] + [
        remote(block(0, 0, 0), block(i, 0, 0), gz_s.at[i], gz_r.at[i], z_peer[i]) for i in range(1, layers)
    ]
    gather_a = [remote(block(i, 0, 0), block(i, 0, 1), ga_s.at[i], ga_r.at[i], a_peer) for i in range(layers)]
    gather_b = [
        [remote(block(i, 0, s), block(i, 0, 2 + s), gb_s.at[i, s], gb_r.at[i, s], b_peer) for s in range(2)]
        for i in range(layers)
    ]
    swap = (0, 2, 1, 3)
    gather_c = [
        [
            remote(block(i, 0, s, wide=False), block(i, 1, swap[s], wide=False), gc_s.at[i, swap[s]], gc_r.at[i, swap[s]], c_peer)
            for s in range(4)
        ]
        for i in range(layers)
    ]
    reduce_p = [remote(part_send.at[i], part_recv.at[i], rp_s.at[i], rp_r.at[i], c_peer) for i in range(layers)]
    reduce_b = [remote(b_send.at[i], b_recv.at[i], rb_s.at[i], rb_r.at[i], b_peer) for i in range(layers)]
    reduce_a = [remote(a_send.at[i], a_recv.at[i], ra_s.at[i], ra_r.at[i], a_peer) for i in range(layers)]
    reduce_z = [None] + [
        remote(z_send.at[i], z_recv.at[i], rz_s.at[i], rz_r.at[i], z_peer[i]) for i in range(1, layers)
    ]
    kept = [None] * layers
    loaded = []

    def first_hop(i):
        if i == 0:
            for j in range(1, layers):
                send(gather_z[j])
        else:
            gather_z[i].wait_recv()
        send(gather_a[i])
        send(gather_b[i][0])
        send(gather_c[i][0])

    def second_hop(i):
        gather_a[i].wait_recv()
        send(gather_b[i][1])
        send(gather_c[i][1])

    def third_hop(i):
        for s in range(2):
            gather_b[i][s].wait_recv()
            send(gather_c[i][2 + s])

    def compute(j):
        pair = (2 * j, 2 * j + 1)
        for i in pair:
            for s in range(4):
                gather_c[i][s].wait_recv()
        if not loaded:
            for load in loads:
                load.wait()
            loaded.append(True)
        count = 4 * tok
        own = rows[2 * j:2 * j + 2, 0, :, 0:half].reshape(2 * count, half)
        other = rows[2 * j:2 * j + 2, 1, :, 0:half].reshape(2 * count, half)
        dot = functools.partial(jnp.dot, preferred_element_type=jnp.float32)
        gated = dot(own, w_gate[0]) + dot(other, w_gate[1])
        lifted = dot(own, w_up[0]) + dot(other, w_up[1])
        hidden = (gated / (1.0 + jnp.exp(-gated)) * lifted).astype(jnp.bfloat16)
        away = dot(hidden, w_down[1]).astype(jnp.bfloat16)
        for i in pair:
            for s in range(4):
                first = (i % 2) * count + s * tok
                part_send[i, swap[s] * tok:(swap[s] + 1) * tok, :] = away[first:first + tok]
            send(reduce_p[i])
        part_own[2 * j:2 * j + 2] = dot(hidden, w_down[0]).astype(jnp.bfloat16).reshape(2, count, half)

    def first_sum(i):
        reduce_p[i].wait_recv()
        names = rows[i, 0, :, half:half + LANES].astype(jnp.float32)
        spots = lax.broadcasted_iota(jnp.int32, names.shape, 1)
        mine = (spots == expert) | (spots == expert + owners) | (spots == expert + 2 * owners)
        weight = jnp.sum(jnp.where(mine, names, 0.0), axis=1, keepdims=True)
        total = (part_own[i].astype(jnp.float32) + part_recv[i].astype(jnp.float32)) * weight
        b_send[i] = total[2 * tok:].astype(jnp.bfloat16)
        send(reduce_b[i])
        part_own[i, 0:2 * tok, :] = total[0:2 * tok].astype(jnp.bfloat16)

    def second_sum(i):
        reduce_b[i].wait_recv()
        total = part_own[i, 0:2 * tok, :].astype(jnp.float32) + b_recv[i].astype(jnp.float32)
        a_send[i] = total[tok:].astype(jnp.bfloat16)
        send(reduce_a[i])
        part_own[i, 0:tok, :] = total[0:tok].astype(jnp.bfloat16)

    def third_sum(i):
        reduce_a[i].wait_recv()
        total = part_own[i, 0:tok, :].astype(jnp.float32) + a_recv[i].astype(jnp.float32)
        if i == 0:
            part_own[i, 0:tok, :] = total.astype(jnp.bfloat16)
        else:
            z_send[i] = total.astype(jnp.bfloat16)
            send(reduce_z[i])

    stages = {"F1": first_hop, "F2": second_hop, "F3": third_hop, "R1": first_sum, "R2": second_sum, "R3": third_sum, "C": compute}
    for name in ORDER:
        stages[name[:-1]](int(name[-1]))

    total = part_own[0, 0:tok, :].astype(jnp.float32)
    for i in range(1, layers):
        reduce_z[i].wait_recv()
        total = total + z_recv[i].astype(jnp.float32)
    out_ref[0] = total.astype(out_ref.dtype)
    for copy in sent:
        copy.wait_send()


def exchange(tokens, gate_weight, up_weight, down_weight, expert_ids, gate_codes):
    layers = lax.axis_size("expert")
    owners = lax.axis_size("dp") * layers
    _, tok, half = tokens.shape
    columns = owners // layers
    units = gate_weight.shape[2]
    vmem, hbm = pl.BlockSpec(memory_space=pltpu.VMEM), pl.BlockSpec(memory_space=pl.ANY)
    dma = pltpu.SemaphoreType.DMA
    bf16 = jnp.bfloat16
    pair = (pltpu.VMEM((layers, tok, half), bf16),) * 2
    return pl.pallas_call(
        functools.partial(exchange_kernel, owners, layers),
        out_shape=jax.ShapeDtypeStruct(tokens.shape, tokens.dtype),
        in_specs=[vmem] * 3 + [hbm] * 3,
        out_specs=vmem,
        scratch_shapes=[
            pltpu.VMEM((layers, 2, columns * tok, half + LANES), bf16),
            pltpu.VMEM((2, half, units), bf16),
            pltpu.VMEM((2, half, units), bf16),
            pltpu.VMEM((2, units, half), bf16),
            pltpu.VMEM((layers, columns * tok, half), bf16),
            pltpu.VMEM((layers, columns * tok, half), bf16),
            pltpu.VMEM((layers, columns * tok, half), bf16),
            pltpu.VMEM((layers, 2 * tok, half), bf16),
            pltpu.VMEM((layers, 2 * tok, half), bf16),
            *pair, *pair,
            dma((2, 3)),
            dma((layers,)), dma((layers,)),
            dma((layers,)), dma((layers,)),
            dma((layers, 2)), dma((layers, 2)),
            dma((layers, 4)), dma((layers, 4)),
            *([dma((layers,))] * 8),
        ],
        compiler_params=pltpu.CompilerParams(
            collective_id=0, has_side_effects=True, vmem_limit_bytes=63 * 1024 * 1024
        ),
    )(tokens, expert_ids.swapaxes(1, 2), gate_codes.swapaxes(1, 2), gate_weight, up_weight, down_weight)


def local(tokens, gate_weight, up_weight, down_weight, expert_ids, gate_codes):
    owners = lax.axis_size("dp") * lax.axis_size("expert")
    tok_rows = tokens.shape[1]
    top_count = expert_ids.shape[2]
    slot_depth = min(tok_rows, max(2, 2 * tok_rows * top_count // owners))
    if (
        slot_depth == tok_rows and lax.axis_size("dp") == 4 and lax.axis_size("expert") == 4
        and lax.axis_size("tensor") == 2 and tokens.shape[0] == 1 and tok_rows % 16 == 0
    ):
        return exchange(tokens, gate_weight, up_weight, down_weight, expert_ids, gate_codes)
    slot_count = owners * slot_depth
    w_gate = gate_weight[0]
    w_up = up_weight[0]
    w_down = down_weight[0]
    slot_numbers = jnp.arange(slot_count, dtype=jnp.int32)
    owner_numbers = jnp.arange(owners, dtype=jnp.int32)
    step_tokens = tokens[0]
    route_ids = expert_ids[0].reshape(tok_rows * top_count)
    onehot = (route_ids[:, None] == owner_numbers[None, :]).astype(jnp.int32)
    before = jnp.cumsum(onehot, axis=0) - onehot
    slot_rank = jnp.sum(before * onehot, axis=1)
    slot_index = route_ids * slot_depth + slot_rank
    select = (slot_index[:, None] == slot_numbers[None, :]).astype(jnp.bfloat16)
    per_token = jnp.sum(select.reshape(tok_rows, top_count, slot_count), axis=1)
    packed = jnp.einsum(
        "ts,td->sd", per_token, step_tokens, preferred_element_type=jnp.float32
    ).astype(jnp.bfloat16)
    packed = packed.reshape(owners, slot_depth, step_tokens.shape[1])
    arrived = lax.all_to_all(packed, ("dp", "expert"), split_axis=0, concat_axis=0, tiled=True)
    owner_rows = arrived.reshape(slot_count, step_tokens.shape[1])
    owner_rows = lax.all_gather(owner_rows, "tensor", axis=1, tiled=True)
    gated = jnp.dot(owner_rows, w_gate, preferred_element_type=jnp.float32)
    lifted = jnp.dot(owner_rows, w_up, preferred_element_type=jnp.float32)
    hidden = (jax.nn.silu(gated) * lifted).astype(jnp.bfloat16)
    partial_value = jnp.dot(hidden, w_down, preferred_element_type=jnp.float32).astype(jnp.bfloat16)
    summed = (
        lax.psum_scatter(partial_value, "tensor", scatter_dimension=1, tiled=True)
        .astype(jnp.float32)
        .astype(jnp.bfloat16)
    )
    half_width = summed.shape[1]
    result = summed.reshape(owners, slot_depth, half_width)
    returned = lax.all_to_all(result, ("dp", "expert"), split_axis=0, concat_axis=0, tiled=True)
    returned = returned.reshape(slot_count, half_width)
    picked = jnp.dot(select, returned, preferred_element_type=jnp.float32)
    codes = gate_codes[0].astype(jnp.float32)
    shares = codes / jnp.sum(codes, axis=1, keepdims=True)
    mixed_rows = jnp.sum(
        picked.reshape(tok_rows, top_count, half_width) * shares[:, :, None], axis=1
    )
    outputs = [mixed_rows.astype(jnp.bfloat16)]
    return jnp.stack(outputs)


def solution(mesh):
    in_specs = (
        P(None, ("dp", "expert"), "tensor"),
        P(("dp", "expert"), None, "tensor"),
        P(("dp", "expert"), None, "tensor"),
        P(("dp", "expert"), "tensor", None),
        P(None, ("dp", "expert"), None),
        P(None, ("dp", "expert"), None),
    )
    out_specs = P(None, ("dp", "expert"), "tensor")
    return jax.shard_map(local, mesh=mesh, in_specs=in_specs, out_specs=out_specs, check_vma=False)
```
